128 devices in a mesh: row: 8 (over x, core), col: 16 (over y, z).
Axes of the slice: x: 4, y: 4, z: 4, core: 2. Of those that a mesh axis runs over, the one named last changes fastest.
Arguments:
- w_rec: bfloat16 [2, 4096, 4, 4096], P(None, 'row', None, 'col'), may hold values from -0.09375 to 0.09375
- w_in: bfloat16 [2, 4096, 4, 4096], P(None, 'row', None, 'col'), may hold values from -0.09375 to 0.09375
- gate_pre: float32 [2, 6, 64, 4, 4096], P(None, None, None, None, 'col'), may hold values from -8 to 8, as said below
- cells: float32 [2, 7, 64, 4096], P(None, None, None, 'col'), may hold values from -6 to 6
- layer_in: bfloat16 [2, 6, 64, 4096], P(None, None, None, 'row'), may hold values from -1 to 1
- h_prev: bfloat16 [2, 6, 64, 4096], P(None, None, None, 'row'), may hold values from -1 to 1
- top_grad: float32 [6, 64, 4096], P(None, None, 'col'), may hold values from -40 to 40
Outputs:
- w_rec_grad: bfloat16 [2, 4096, 4, 4096], P(None, 'row', None, 'col')
- w_in_grad: bfloat16 [2, 4096, 4, 4096], P(None, 'row', None, 'col')
- input_grad: float32 [6, 64, 4096], P(None, None, 'col')
The draws below stay inside these ranges and needn't reach their ends.
Inputs may be any that keep to these rules, and one draw needn't show every extreme that they name: `gate_pre`: dimension 3 holds the input, forget, candidate and output gates in that order.
All inputs are finite; a program needn't handle non-finite values.
Results may differ from the reference program's by a relative error of at most 0.0051.
Values sent between devices are 32-bit elements; how exact they have to be, the bound alone decides.
A program may use at most 128 MiB of HBM per device.

```python
import math
import jax
import jax.numpy as jnp
from jax import lax

WIDTH = 4096
LAYERS = 2
STEPS = 6
BATCH = 64


def draw_gate_pre(key, part):
    first, second = jax.random.split(jax.random.fold_in(key, 11), 2)
    shape = (LAYERS, STEPS, BATCH, 4, WIDTH)
    noise = jax.random.normal(first, shape, jnp.float32)
    offset = jax.random.uniform(second, (LAYERS, 1, 1, 1, WIDTH), jnp.float32, -1.0, 5.0)
    chosen = (jnp.arange(4) == 1).reshape(1, 1, 1, 4, 1)
    values = jnp.where(chosen, offset + 0.7 * noise, 1.5 * noise)
    return jnp.clip(values, -8.0, 8.0)


def draw_top_grad(key, part):
    first, second, third = jax.random.split(jax.random.fold_in(key, 23), 3)
    shape = (STEPS, BATCH, WIDTH)
    phases = jax.random.uniform(first, (2,), jnp.float32, 0.0, 2.0 * math.pi)
    where_unit = jnp.arange(WIDTH).astype(jnp.float32) / WIDTH
    envelope = 1.2 * jnp.sin(2.0 * math.pi * where_unit + phases[0]) + 0.6 * jnp.sin(6.0 * math.pi * where_unit + phases[1])
    factor = 2.0 * jnp.exp(envelope)
    base = jax.random.normal(second, shape, jnp.float32)
    return jnp.clip(base * factor, -40.0, 40.0)


def steps_of(rng, shape, shards, smallest, largest):
    level = 1.0
    for axis_at, blocks in shards:
        heights = jax.random.uniform(jax.random.fold_in(jax.random.fold_in(rng, 6), axis_at), (blocks,), jnp.float32, smallest / len(shards), largest / len(shards))
        level = level * jnp.repeat(jnp.exp(heights), shape[axis_at] // blocks).reshape((-1,) + (1,) * (len(shape) - 1 - axis_at))
    return level


def scatter_about(stream_key, extent, deviation, bound, shards=(), kind=jnp.bfloat16):
    array = deviation * jax.random.normal(stream_key, extent, jnp.float32)
    if shards:
        array = array * steps_of(stream_key, extent, shards, -0.22, 0.18)
    return jnp.clip(array, -bound, bound).astype(kind)


def setup_inputs(seed: int = 0) -> dict:
    streams_of = jax.random.split(jax.random.key(seed), 8)
    return {
        "w_rec": scatter_about(streams_of[0], (LAYERS, WIDTH, 4, WIDTH), WIDTH ** -0.5, 0.09375, ((1, 8), (3, 16))),
        "w_in": scatter_about(streams_of[1], (LAYERS, WIDTH, 4, WIDTH), WIDTH ** -0.5, 0.09375, ((1, 8), (3, 16))),
        "gate_pre": draw_gate_pre(jax.random.fold_in(streams_of[7], 71), 0),
        "cells": scatter_about(streams_of[3], (LAYERS, STEPS + 1, BATCH, WIDTH), 1.0, 6.0, ((3, 16),), jnp.float32),
        "layer_in": jnp.clip(jax.random.uniform(streams_of[4], (LAYERS, STEPS, BATCH, WIDTH), jnp.float32, -1.0, 1.0) * steps_of(streams_of[4], (LAYERS, STEPS, BATCH, WIDTH), ((3, 8),), -0.4, 0.0), -1.0, 1.0).astype(jnp.bfloat16),
        "h_prev": jnp.clip(jax.random.uniform(streams_of[5], (LAYERS, STEPS, BATCH, WIDTH), jnp.float32, -1.0, 1.0) * steps_of(streams_of[5], (LAYERS, STEPS, BATCH, WIDTH), ((3, 8),), -0.4, 0.0), -1.0, 1.0).astype(jnp.bfloat16),
        "top_grad": draw_top_grad(jax.random.fold_in(streams_of[7], 71), 0),
    }


def cell_backward(preact, cell_prev, cell_now, hid_grad, cell_carry):
    in_gate = jax.nn.sigmoid(preact[:, 0])
    forget = jax.nn.sigmoid(preact[:, 1])
    cand_gate = jnp.tanh(preact[:, 2])
    out_gate = jax.nn.sigmoid(preact[:, 3])
    tanh_cell = jnp.tanh(cell_now)
    cell_grad = cell_carry + hid_grad * out_gate * (1.0 - tanh_cell * tanh_cell)
    grad_in = cell_grad * cand_gate * in_gate * (1.0 - in_gate)
    grad_forget = cell_grad * cell_prev * forget * (1.0 - forget)
    grad_cand = cell_grad * in_gate * (1.0 - cand_gate * cand_gate)
    grad_out = hid_grad * tanh_cell * out_gate * (1.0 - out_gate)
    gate_grads = jnp.stack([grad_in, grad_forget, grad_cand, grad_out], axis=1).astype(jnp.bfloat16)
    return (gate_grads, cell_grad * forget)

def reference(w_rec, w_in, gate_pre, cells, layer_in, h_prev, top_grad):
    incoming = top_grad
    rec_grads = [None] * LAYERS
    in_grads = [None] * LAYERS
    sumsq = jnp.zeros((), jnp.float32)
    for layer in range(LAYERS - 1, -1, -1):
        rec_flat = w_rec[layer].reshape(WIDTH, 4 * WIDTH)

        def advance(carry, inputs, rec_flat=rec_flat):
            rec_carry, cell_carry = carry
            preact, cell_prev, cell_now, outside = inputs
            gate_grads, cell_next = cell_backward(preact, cell_prev, cell_now, outside + rec_carry, cell_carry)
            recurrent = jnp.dot(gate_grads.reshape(BATCH, 4 * WIDTH), rec_flat.T, preferred_element_type=jnp.float32)
            return ((recurrent, cell_next), gate_grads)
        zeros = jnp.zeros((BATCH, WIDTH), jnp.float32)
        carried, stacked = lax.scan(advance, (zeros, zeros), (gate_pre[layer], cells[layer, :STEPS], cells[layer, 1:], incoming), reverse=True)
        flat = stacked.reshape(STEPS * BATCH, 4 * WIDTH)
        incoming = jnp.dot(flat, w_in[layer].reshape(WIDTH, 4 * WIDTH).T, preferred_element_type=jnp.float32).reshape(STEPS, BATCH, WIDTH)
        raw_rec = jnp.dot(h_prev[layer].reshape(STEPS * BATCH, WIDTH).T, flat, preferred_element_type=jnp.float32)
        raw_in = jnp.dot(layer_in[layer].reshape(STEPS * BATCH, WIDTH).T, flat, preferred_element_type=jnp.float32)
        sumsq = sumsq + jnp.sum(raw_rec * raw_rec) + jnp.sum(raw_in * raw_in)
        rec_grads[layer] = raw_rec
        in_grads[layer] = raw_in
    scale = 1.0 / jnp.maximum(jnp.sqrt(sumsq / (8.0 * LAYERS * WIDTH * WIDTH)), 0.05)
    w_rec_grad = jnp.stack([(rec_grads[layer] * scale).reshape(WIDTH, 4, WIDTH) for layer in range(LAYERS)]).astype(jnp.bfloat16)
    w_in_grad = jnp.stack([(in_grads[layer] * scale).reshape(WIDTH, 4, WIDTH) for layer in range(LAYERS)]).astype(jnp.bfloat16)
    return (w_rec_grad, w_in_grad, incoming)
```

```python
import jax
import jax.numpy as jnp
from jax import lax
from jax.experimental import pallas as pl
from jax.experimental.pallas import tpu as pltpu
from jax.sharding import Mesh
from jax.sharding import PartitionSpec as P

COL = ("col_0", "col_1")
ROW = ("row_0", "row_1")
MESH = pl.DeviceIdType.MESH
F32 = jnp.float32
BF16 = jnp.bfloat16
NORM = 268435456.0
ROWS = 8
COLS = 16
T = 6
B = 64
J = 512
U = 256
PIECE = 16
IPIECE = 8


def dev(r, c):
    return (r // 2, r % 2, c // 4, c % 4)


def push(src, dst, send_sem, recv_sem, where):
    pltpu.make_async_remote_copy(
        src_ref=src, dst_ref=dst, send_sem=send_sem, recv_sem=recv_sem,
        device_id=where, device_id_type=MESH,
    ).start()


def drain(ref, sem):
    pltpu.make_async_copy(ref, ref, sem).wait()


def nt(a, b):
    return lax.dot_general(a, b, (((1,), (1,)), ((), ())), preferred_element_type=F32)


def tn(a, b):
    return lax.dot_general(a, b, (((0,), (0,)), ((), ())), preferred_element_type=F32)


def kernel(
    w_rec, w_in, gate_pre, cells, layer_in, h_prev, top_grad,
    o_rec, o_in, o_inp,
    wraw, tmp, wk, gp, cl, li, hp, tg, dgs, acc, fac, carry,
    sb, rb, hb, sbi, rbi, gbi, gs, ps, rs,
    ld, st, rs_s, rs_r, ag_s, ag_r, ris_s, ris_r, ia_s, ia_r, gs_s, gs_r, ps_s, ps_r,
):
    r = lax.axis_index("row_0") * 2 + lax.axis_index("row_1")
    c = lax.axis_index("col_0") * 4 + lax.axis_index("col_1")
    mine = r == c // 2
    own = (c % 2) * ROWS + r

    loads = [
        (gate_pre, gp), (cells, cl), (top_grad, tg),
        (w_rec.at[1], wraw.at[2]), (w_in.at[1], wraw.at[3]),
        (w_rec.at[0], wraw.at[0]), (w_in.at[0], wraw.at[1]),
        (h_prev, hp), (layer_in, li),
    ]
    copies = [pltpu.make_async_copy(a, b, ld.at[i]) for i, (a, b) in enumerate(loads)]
    for copy in copies:
        copy.start()

    barrier = pltpu.get_barrier_semaphore()
    for i in range(1, ROWS):
        pl.semaphore_signal(barrier, inc=1, device_id=dev((r + i) % ROWS, c), device_id_type=MESH)
    for i in range(COLS):
        @pl.when(jnp.logical_or(r != c // 2, c != i))
        def _():
            pl.semaphore_signal(barrier, inc=1, device_id=dev(c // 2, i), device_id_type=MESH)

    def relayout(m):
        tmp[...] = wraw[m].astype(F32)
        for i in range(8):
            wk[m, :, pl.ds(i * 128, 128)] = tmp[pl.ds(i, J, stride=8), :].astype(BF16)

    def factors(layer, t):
        for ut in range(2):
            lanes = pl.ds(ut * 128, 128)
            gi = jax.nn.sigmoid(gp[layer, t, :, ut * 4 + 0, :])
            gf = jax.nn.sigmoid(gp[layer, t, :, ut * 4 + 1, :])
            gc = jnp.tanh(gp[layer, t, :, ut * 4 + 2, :])
            go = jax.nn.sigmoid(gp[layer, t, :, ut * 4 + 3, :])
            th = jnp.tanh(cl[layer, t + 1, :, lanes])
            fac[layer, 0, :, lanes] = go * (1.0 - th * th)
            fac[layer, 1, :, lanes] = gc * gi * (1.0 - gi)
            fac[layer, 2, :, lanes] = cl[layer, t, :, lanes] * gf * (1.0 - gf)
            fac[layer, 3, :, lanes] = gi * (1.0 - gc * gc)
            fac[layer, 4, :, lanes] = th * go * (1.0 - go)
            fac[layer, 5, :, lanes] = gf

    def cell(layer, t, hid):
        grad = carry[layer] + hid * fac[layer, 0]
        carry[layer] = grad * fac[layer, 5]
        parts = [grad * fac[layer, 1], grad * fac[layer, 2], grad * fac[layer, 3], hid * fac[layer, 4]]
        for ut in range(2):
            for k in range(4):
                dgs[layer, t, :, pl.ds((ut * 4 + k) * 128, 128)] = (
                    parts[k][:, ut * 128 : ut * 128 + 128].astype(BF16)
                )

    def scatter(src, dst, send_sem, recv_sem):
        for i in range(2 * ROWS):
            q = (r + [4, 5, 2, 3, 6, 7, 0, 1][i // 2]) % ROWS
            h = i % 2
            @pl.when(jnp.logical_or(q != r, 2 * r + h != c))
            def _():
                push(src.at[h * ROWS + q], dst.at[c], send_sem, recv_sem, dev(q, 2 * r + h))

    def scatter_wait(ref, sem):
        @pl.when(mine)
        def _():
            drain(ref.at[pl.ds(0, COLS - 1)], sem)

        @pl.when(jnp.logical_not(mine))
        def _():
            drain(ref, sem)

    def gather(src, dst, send_sem, recv_sem):
        for i in [4, 5, 2, 3, 6, 7, 1]:
            push(src, dst.at[r], send_sem, recv_sem, dev((r + i) % ROWS, c))

    def gather_wait(ref, sem):
        drain(ref.at[pl.ds(0, ROWS - 1)], sem)

    def total(ref):
        out = ref[0]
        for i in range(1, COLS):
            out = out + ref[i]
        return out

    def keep_own(src, dst):
        @pl.when(mine)
        def _():
            dst[c] = src[own]

    def weight_grads(layer, t):
        for s, left in enumerate((hp, li)):
            for i in range(4):
                prod = tn(left[layer, t], dgs[layer, t, :, pl.ds(i * 256, 256)])
                for q in range(2):
                    where = (2 * layer + s, pl.ds(2 * i + q, J, stride=8))
                    acc[where] = acc[where] + prod[:, q * 128 : q * 128 + 128]

    def input_send(d, t):
        prod = nt(dgs[0, t], wk[1])
        for h in range(2):
            sbi[d, pl.ds(h * ROWS, ROWS)] = prod[:, h * U : h * U + U].reshape(ROWS, IPIECE, U)
        keep_own(sbi.at[d], rbi.at[d])
        scatter(sbi.at[d], rbi.at[d], ris_s.at[d], ris_r.at[d])

    def input_sum(d, t):
        scatter_wait(rbi.at[d], ris_r.at[d])
        gbi[t, r] = total(rbi.at[d])
        gather(gbi.at[t, r], gbi.at[t], ia_s.at[t], ia_r.at[t])

    zero_piece = jnp.zeros((B, U), F32)
    hb[0] = jnp.zeros((ROWS, PIECE, U), F32)
    for layer in range(2):
        carry[layer] = zero_piece
    for n in range(6):
        fac[0, n] = zero_piece

    def clear(i, x):
        acc[:, pl.ds(pl.multiple_of(i * 256, 256), 256), :] = jnp.zeros((4, 256, 128), F32)
        return x

    lax.fori_loop(0, 16, clear, 0)
    copies[0].wait()
    copies[1].wait()
    copies[2].wait()
    factors(1, T - 1)
    copies[3].wait()
    relayout(2)
    copies[4].wait()
    relayout(3)

    @pl.when(mine)
    def _():
        pl.semaphore_wait(barrier, ROWS - 1 + COLS - 1)

    @pl.when(jnp.logical_not(mine))
    def _():
        pl.semaphore_wait(barrier, ROWS - 1 + COLS)

    def diagonal(d, x):
        t1 = T - 1 - d
        t0 = T - d
        cell(1, t1, hb[d, pl.ds(0, 4)].reshape(B, U) + tg[t1])
        cell(0, t0, hb[d, pl.ds(4, 4)].reshape(B, U))
        up = nt(dgs[1, t1], wk[2])
        down = nt(dgs[1, t1], wk[3])
        for h in range(2):
            sb[d, pl.ds(h * ROWS, 4)] = up[:, h * U : h * U + U].reshape(4, PIECE, U)
            sb[d, pl.ds(h * ROWS + 4, 4)] = down[:, h * U : h * U + U].reshape(4, PIECE, U)

        @pl.when(d > 0)
        def _():
            more = nt(dgs[0, t0], wk[0])
            for h in range(2):
                at = (d, pl.ds(h * ROWS + 4, 4))
                sb[at] = sb[at] + more[:, h * U : h * U + U].reshape(4, PIECE, U)

        keep_own(sb.at[d], rb.at[d])
        scatter(sb.at[d], rb.at[d], rs_s.at[d], rs_r.at[d])

        @pl.when(d == 0)
        def _():
            copies[5].wait()
            relayout(0)
            copies[6].wait()
            relayout(1)
            copies[7].wait()
            copies[8].wait()

        @pl.when(d > 0)
        def _():
            input_send(d, t0)

        factors(0, T - 1 - d)

        @pl.when(d < T - 1)
        def _():
            factors(1, T - 2 - d)

        weight_grads(1, t1)

        @pl.when(d > 0)
        def _():
            weight_grads(0, t0)

        scatter_wait(rb.at[d], rs_r.at[d])
        hb[d + 1, r] = total(rb.at[d])
        gather(hb.at[d + 1, r], hb.at[d + 1], ag_s.at[d], ag_r.at[d])

        @pl.when(d > 0)
        def _():
            input_sum(d, t0)

        gather_wait(hb.at[d + 1], ag_r.at[d])
        return x

    lax.fori_loop(0, T, diagonal, 0)

    cell(0, 0, hb[T, pl.ds(4, 4)].reshape(B, U))
    input_send(T, 0)
    weight_grads(0, 0)

    def squares(i, x):
        part = acc[:, pl.ds(pl.multiple_of(i * 256, 256), 256), :]
        return x + jnp.sum((part * part).reshape(128, 8, 128), axis=0)

    gs[r] = lax.fori_loop(0, 16, squares, jnp.zeros((8, 128), F32))
    gather(gs.at[r], gs, gs_s, gs_r)
    gather_wait(gs, gs_r)
    row_sum = gs[0]
    for i in range(1, ROWS):
        row_sum = row_sum + gs[i]
    ps[...] = row_sum

    @pl.when(mine)
    def _():
        rs[c] = row_sum

    for i in range(2 * ROWS):
        q = (r + [4, 5, 2, 3, 6, 7, 0, 1][i // 2]) % ROWS
        h = i % 2
        @pl.when(jnp.logical_or(q != r, 2 * r + h != c))
        def _():
            push(ps, rs.at[c], ps_s, ps_r, dev(q, 2 * r + h))

    input_sum(T, 0)
    scatter_wait(rs, ps_r)
    sumsq = jnp.sum(total(rs), keepdims=True)
    scale = 1.0 / jnp.maximum(jnp.sqrt(sumsq / NORM), 0.05)

    writes = []
    for m, out in enumerate((o_rec.at[0], o_in.at[0], o_rec.at[1], o_in.at[1])):
        for q in range(2):
            def finish(i, x, m=m, q=q):
                at = pl.ds(pl.multiple_of(q * 2048 + i * 256, 256), 256)
                wraw[m, at, :] = (acc[m, at, :] * scale).astype(BF16)
                return x

            lax.fori_loop(0, 8, finish, 0)
            at = pl.ds(q * 2048, 2048)
            copy = pltpu.make_async_copy(wraw.at[m, at], out.at[at], st.at[m])
            copy.start()
            writes.append(copy)

    for t in range(T - 1, -1, -1):
        gather_wait(gbi.at[t], ia_r.at[t])
    copy = pltpu.make_async_copy(gbi, o_inp, st.at[4])
    copy.start()
    writes.append(copy)

    def sent(d, x):
        scatter_wait(sb.at[d], rs_s.at[d])
        gather_wait(hb.at[d + 1], ag_s.at[d])
        scatter_wait(sbi.at[d + 1], ris_s.at[d + 1])
        gather_wait(gbi.at[d], ia_s.at[d])
        return x

    lax.fori_loop(0, T, sent, 0)
    gather_wait(gs, gs_s)
    scatter_wait(rs, ps_s)
    for m in range(4):
        drain(wraw.at[m], st.at[m])
    writes[-1].wait()


def local(w_rec, w_in, gate_pre, cells, layer_in, h_prev, top_grad):
    def tiles(w):
        lead = w.shape[:-2]
        axes = tuple(range(len(lead)))
        n = len(lead)
        return w.reshape(lead + (4, 2, 128)).transpose(axes + (n + 1, n, n + 2))

    any_space = pl.BlockSpec(memory_space=pl.ANY)
    vmem = pltpu.VMEM
    dma = pltpu.SemaphoreType.DMA
    rec, inp, igrad = pl.pallas_call(
        kernel,
        out_shape=(
            jax.ShapeDtypeStruct((2, 8 * J, 128), BF16),
            jax.ShapeDtypeStruct((2, 8 * J, 128), BF16),
            jax.ShapeDtypeStruct((T, ROWS, IPIECE, U), F32),
        ),
        in_specs=[any_space] * 7,
        out_specs=(any_space,) * 3,
        scratch_shapes=[
            vmem((4, 8 * J, 128), BF16),
            vmem((8 * J, 128), F32),
            vmem((4, J, 4 * U), BF16),
            vmem((2, T, B, 8, 128), F32),
            vmem((2, T + 1, B, U), F32),
            vmem((2, T, B, J), BF16),
            vmem((2, T, B, J), BF16),
            vmem((T, B, U), F32),
            vmem((2, T + 1, B, 4 * U), BF16),
            vmem((4, 8 * J, 128), F32),
            vmem((2, 6, B, U), F32),
            vmem((2, B, U), F32),
            vmem((T, 2 * ROWS, PIECE, U), F32),
            vmem((T, COLS, PIECE, U), F32),
            vmem((T + 1, ROWS, PIECE, U), F32),
            vmem((T + 1, 2 * ROWS, IPIECE, U), F32),
            vmem((T + 1, COLS, IPIECE, U), F32),
            vmem((T, ROWS, IPIECE, U), F32),
            vmem((ROWS, 8, 128), F32),
            vmem((8, 128), F32),
            vmem((COLS, 8, 128), F32),
            dma((9,)), dma((5,)),
            dma((T,)), dma((T,)), dma((T,)), dma((T,)),
            dma((T + 1,)), dma((T + 1,)), dma((T,)), dma((T,)),
            dma, dma, dma, dma,
        ],
        compiler_params=pltpu.CompilerParams(
            collective_id=0, has_side_effects=True, vmem_limit_bytes=60 * 1024 * 1024
        ),
    )(
        tiles(w_rec).reshape(2, 8 * J, 128),
        tiles(w_in).reshape(2, 8 * J, 128),
        tiles(gate_pre).reshape(2, T, B, 8, 128),
        cells, layer_in, h_prev, top_grad,
    )

    def back(w):
        return w.reshape(2, J, 2, 4, 128).transpose(0, 1, 3, 2, 4).reshape(2, J, 4, U)

    return back(rec), back(inp), igrad.reshape(T, B, U)


def solution(mesh):
    torus = Mesh(mesh.devices.reshape(4, 2, 4, 4), ("row_0", "row_1", "col_0", "col_1"))
    placed = (
        P(None, ROW, None, COL),
        P(None, ROW, None, COL),
        P(None, None, None, None, COL),
        P(None, None, None, COL),
        P(None, None, None, ROW),
        P(None, None, None, ROW),
        P(None, None, COL),
    )
    return jax.shard_map(
        local,
        mesh=torus,
        in_specs=placed,
        out_specs=(P(None, ROW, None, COL), P(None, ROW, None, COL), P(None, None, COL)),
        check_vma=False,
    )
```

```python
import jax
import jax.numpy as jnp
from jax import lax
from jax.experimental import pallas as pl
from jax.experimental.pallas import tpu as pltpu
from jax.sharding import Mesh
from jax.sharding import PartitionSpec as P

COL = ("col_0", "col_1")
ROW = ("row_0", "row_1")
MESH = pl.DeviceIdType.MESH
F32 = jnp.float32
BF16 = jnp.bfloat16
NORM = 268435456.0
ROWS = 8
COLS = 16
T = 6
B = 64
J = 512
U = 256
VMEM_LIMIT = 44 * 1024 * 1024
PIECE = 8


def dev(r, c):
    return (r // 2, r % 2, c // 4, c % 4)


def push(src, dst, send_sem, recv_sem, where):
    pltpu.make_async_remote_copy(
        src_ref=src, dst_ref=dst, send_sem=send_sem, recv_sem=recv_sem,
        device_id=where, device_id_type=MESH,
    ).start()


def drain(ref, sem):
    pltpu.make_async_copy(ref, ref, sem).wait()


def nt(a, b):
    return lax.dot_general(a, b, (((1,), (1,)), ((), ())), preferred_element_type=F32)


def tn(a, b):
    return lax.dot_general(a, b, (((0,), (0,)), ((), ())), preferred_element_type=F32)


def kernel(
    w_rec, w_in, gate_pre, cells, layer_in, h_prev, top_grad,
    a_rec, a_in, o_inp, o_scale,
    wraw, tmp, wk, gp, cl, li, hp, tg, dgs, fac, carry, sq,
    sb, rb, hb, gs, ps, rs,
    ld, rs_s, rs_r, ag_s, ag_r, gs_s, gs_r, ps_s, ps_r,
):
    r = lax.axis_index("row_0") * 2 + lax.axis_index("row_1")
    c = lax.axis_index("col_0") * 4 + lax.axis_index("col_1")
    mine = r == c // 2
    own = (c % 2) * ROWS + r
    grads = (a_rec, a_in)

    barrier = pltpu.get_barrier_semaphore()
    for i in range(1, ROWS):
        pl.semaphore_signal(barrier, inc=1, device_id=dev((r + i) % ROWS, c), device_id_type=MESH)
    for i in range(COLS):
        @pl.when(jnp.logical_or(r != c // 2, c != i))
        def _():
            pl.semaphore_signal(barrier, inc=1, device_id=dev(c // 2, i), device_id_type=MESH)

    last = pl.ds(T - 1, 1)
    rest = pl.ds(0, T - 1)
    loads = [
        (gate_pre.at[1, last], gp.at[1, last]), (cells.at[1], cl.at[1]), (w_rec.at[1], wraw.at[2]),
        (top_grad, tg), (w_in.at[1], wraw.at[3]),
        (w_rec.at[0], wraw.at[0]), (w_in.at[0], wraw.at[1]),
        (gate_pre.at[0], gp.at[0]), (gate_pre.at[1, rest], gp.at[1, rest]), (cells.at[0], cl.at[0]),
        (h_prev, hp), (layer_in, li),
    ]
    copies = [pltpu.make_async_copy(p, q, ld.at[i]) for i, (p, q) in enumerate(loads)]
    for copy in copies:
        copy.start()

    def relayout(m):
        tmp[...] = wraw[m].astype(F32)
        for i in range(8):
            wk[m, :, pl.ds(i * 128, 128)] = tmp[pl.ds(i, J, stride=8), :].astype(BF16)

    def factors(layer, t):
        for ut in range(2):
            lanes = pl.ds(ut * 128, 128)
            gi = jax.nn.sigmoid(gp[layer, t, :, ut * 4 + 0, :])
            gf = jax.nn.sigmoid(gp[layer, t, :, ut * 4 + 1, :])
            gc = jnp.tanh(gp[layer, t, :, ut * 4 + 2, :])
            go = jax.nn.sigmoid(gp[layer, t, :, ut * 4 + 3, :])
            th = jnp.tanh(cl[layer, t + 1, :, lanes])
            fac[layer, 0, :, lanes] = go * (1.0 - th * th)
            fac[layer, 1, :, lanes] = gc * gi * (1.0 - gi)
            fac[layer, 2, :, lanes] = cl[layer, t, :, lanes] * gf * (1.0 - gf)
            fac[layer, 3, :, lanes] = gi * (1.0 - gc * gc)
            fac[layer, 4, :, lanes] = th * go * (1.0 - go)
            fac[layer, 5, :, lanes] = gf

    def cell(layer, t, hid):
        grad = carry[layer] + hid * fac[layer, 0]
        carry[layer] = grad * fac[layer, 5]
        parts = [grad * fac[layer, 1], grad * fac[layer, 2], grad * fac[layer, 3], hid * fac[layer, 4]]
        for ut in range(2):
            for k in range(4):
                dgs[layer, t, :, pl.ds((ut * 4 + k) * 128, 128)] = (
                    parts[k][:, ut * 128 : ut * 128 + 128].astype(BF16)
                )

    def to_each(send):
        for i in range(2 * ROWS):
            q = (r + [4, 5, 2, 3, 6, 7, 0, 1][i // 2]) % ROWS
            h = i % 2
            @pl.when(jnp.logical_or(q != r, 2 * r + h != c))
            def _():
                send(h * ROWS + q, dev(q, 2 * r + h))

    def scatter(ch, s):
        @pl.when(mine)
        def _():
            rb[ch, s, c] = sb[ch, s, own]

        to_each(lambda piece, where: push(
            sb.at[ch, s, piece], rb.at[ch, s, c], rs_s.at[ch, s], rs_r.at[ch, s], where))

    def scatter_wait(ref, sem):
        @pl.when(mine)
        def _():
            drain(ref.at[pl.ds(0, COLS - 1)], sem)

        @pl.when(jnp.logical_not(mine))
        def _():
            drain(ref, sem)

    def gather(src, dst, send_sem, recv_sem):
        for i in [4, 5, 2, 3, 6, 7, 1]:
            push(src, dst.at[r], send_sem, recv_sem, dev((r + i) % ROWS, c))

    def gather_wait(ref, sem):
        drain(ref.at[pl.ds(0, ROWS - 1)], sem)

    def total(ref):
        terms = [ref[i] for i in range(COLS)]
        while len(terms) > 1:
            terms = [p + q for p, q in zip(terms[::2], terms[1::2])]
        return terms[0]

    def pass_on(ch, s, to):
        scatter_wait(rb.at[ch, s], rs_r.at[ch, s])
        hb[ch, to, r] = total(rb.at[ch, s])
        gather(hb.at[ch, to, r], hb.at[ch, to], ag_s.at[ch, to], ag_r.at[ch, to])

    def store(ch, s, prod, add=False):
        for h in range(2):
            at = (ch, s, pl.ds(h * ROWS, ROWS))
            piece = prod[:, h * U : h * U + U].reshape(ROWS, PIECE, U)
            sb[at] = sb[at] + piece if add else piece

    def folded(x):
        return jnp.sum(x.reshape(-1, 64, 128), axis=0)

    def weight_grads(layer, t, square=False):
        for s, left in enumerate((hp, li)):
            for i in range(4):
                prod = tn(left[layer, t], dgs[layer, t, :, pl.ds(i * 256, 256)])
                for q in range(2):
                    where = (layer, pl.ds(2 * i + q, J, stride=8))
                    full = grads[s][where] + prod[:, q * 128 : q * 128 + 128]
                    grads[s][where] = full
                    if square:
                        sq[...] = sq[...] + folded(full * full)

    def hidden(ch, d):
        return hb[ch, d].reshape(B, U)

    copies[0].wait()
    copies[1].wait()
    factors(1, T - 1)
    copies[2].wait()
    relayout(2)
    copies[3].wait()
    copies[4].wait()
    relayout(3)
    zero = jnp.zeros((B, U), F32)
    for layer in range(2):
        carry[layer] = zero
        hb[layer, 0] = jnp.zeros((ROWS, PIECE, U), F32)
    for n in range(6):
        fac[0, n] = zero

    @pl.when(mine)
    def _():
        pl.semaphore_wait(barrier, ROWS - 1 + COLS - 1)

    @pl.when(jnp.logical_not(mine))
    def _():
        pl.semaphore_wait(barrier, ROWS - 1 + COLS)

    def diagonal(d, x):
        t1 = T - 1 - d
        t0 = T - d

        @pl.when(d > 0)
        def _():
            gather_wait(hb.at[0, d], ag_r.at[0, d])

        cell(1, t1, hidden(0, d) + tg[t1])

        @pl.when(d < T - 1)
        def _():
            store(0, d, nt(dgs[1, t1], wk[2]))
            scatter(0, d)

        store(1, d, nt(dgs[1, t1], wk[3]))

        @pl.when(d > 0)
        def _():
            gather_wait(hb.at[1, d], ag_r.at[1, d])

        cell(0, t0, hidden(1, d))

        @pl.when(d > 0)
        def _():
            store(1, d, nt(dgs[0, t0], wk[0]), add=True)

        scatter(1, d)

        @pl.when(d == 0)
        def _():
            for n in range(2):
                for i in range(8):
                    for layer in range(2):
                        grads[n][layer, pl.ds(i * J, J), :] = jnp.zeros((J, 128), F32)
            copies[5].wait()
            relayout(0)
            copies[6].wait()
            relayout(1)
            for copy in copies[7:]:
                copy.wait()

        factors(0, T - 1 - d)

        @pl.when(d < T - 1)
        def _():
            factors(1, T - 2 - d)

        weight_grads(1, t1)

        @pl.when(d > 0)
        def _():
            store(2, t0, nt(dgs[0, t0], wk[1]))

        @pl.when(d < T - 1)
        def _():
            pass_on(0, d, d + 1)

        pass_on(1, d, d + 1)

        @pl.when(d > 0)
        def _():
            scatter(2, t0)

        @pl.when(d > 0)
        def _():
            weight_grads(0, t0)

        @pl.when(d > 1)
        def _():
            pass_on(2, t0 + 1, t0 + 1)

        return x

    lax.fori_loop(0, T, diagonal, 0)

    def squares(i, x):
        at = pl.ds(pl.multiple_of(i * 512, 512), 512)
        for n in range(2):
            part = grads[n][1, at, :]
            x = x + folded(part * part)
        return x

    sq[...] = lax.fori_loop(0, 8, squares, jnp.zeros((64, 128), F32))
    gather_wait(hb.at[1, T], ag_r.at[1, T])
    cell(0, 0, hidden(1, T))
    store(2, 0, nt(dgs[0, 0], wk[1]))
    scatter(2, 0)
    weight_grads(0, 0, square=True)
    gs[r] = jnp.sum(sq[...].reshape(8, 8, 128), axis=0)
    gather(gs.at[r], gs, gs_s, gs_r)
    pass_on(2, 1, 1)
    gather_wait(gs, gs_r)
    row_sum = gs[0]
    for i in range(1, ROWS):
        row_sum = row_sum + gs[i]
    ps[...] = row_sum

    @pl.when(mine)
    def _():
        rs[c] = row_sum

    to_each(lambda piece, where: push(ps, rs.at[c], ps_s, ps_r, where))
    pass_on(2, 0, 0)
    scatter_wait(rs, ps_r)
    sumsq = jnp.sum(total(rs), keepdims=True)
    scale = 1.0 / jnp.maximum(jnp.sqrt(sumsq / NORM), 0.05)
    o_scale[...] = jnp.broadcast_to(scale, (8, 128))

    def sent(d, x):
        @pl.when(d < T - 1)
        def _():
            scatter_wait(sb.at[0, d], rs_s.at[0, d])
            gather_wait(hb.at[0, d + 1], ag_s.at[0, d + 1])

        scatter_wait(sb.at[1, d], rs_s.at[1, d])
        gather_wait(hb.at[1, d + 1], ag_s.at[1, d + 1])
        scatter_wait(sb.at[2, d], rs_s.at[2, d])
        gather_wait(hb.at[2, d], ag_s.at[2, d])
        gather_wait(hb.at[2, d], ag_r.at[2, d])
        return x

    lax.fori_loop(0, T, sent, 0)
    gather_wait(gs, gs_s)
    scatter_wait(rs, ps_s)
    o_inp[...] = hb[2, pl.ds(0, T)]


def local(w_rec, w_in, gate_pre, cells, layer_in, h_prev, top_grad):
    def tiles(w):
        lead = w.shape[:-2]
        axes = tuple(range(len(lead)))
        n = len(lead)
        return w.reshape(lead + (4, 2, 128)).transpose(axes + (n + 1, n, n + 2))

    any_space = pl.BlockSpec(memory_space=pltpu.HBM)
    in_vmem = pl.BlockSpec(memory_space=pltpu.VMEM)
    vmem = pltpu.VMEM
    dma = pltpu.SemaphoreType.DMA
    rec, inp, igrad, scale = pl.pallas_call(
        kernel,
        out_shape=(
            vmem((2, 8 * J, 128), F32),
            vmem((2, 8 * J, 128), F32),
            vmem((T, ROWS, PIECE, U), F32),
            vmem((8, 128), F32),
        ),
        in_specs=[any_space] * 7,
        out_specs=(in_vmem,) * 4,
        scratch_shapes=[
            vmem((4, 8 * J, 128), BF16),
            vmem((8 * J, 128), F32),
            vmem((4, J, 4 * U), BF16),
            vmem((2, T, B, 8, 128), F32),
            vmem((2, T + 1, B, U), F32),
            vmem((2, T, B, J), BF16),
            vmem((2, T, B, J), BF16),
            vmem((T, B, U), F32),
            vmem((2, T + 1, B, 4 * U), BF16),
            vmem((2, 6, B, U), F32),
            vmem((2, B, U), F32),
            vmem((64, 128), F32),
            vmem((3, T, 2 * ROWS, PIECE, U), F32),
            vmem((3, T, COLS, PIECE, U), F32),
            vmem((3, T + 1, ROWS, PIECE, U), F32),
            vmem((ROWS, 8, 128), F32),
            vmem((8, 128), F32),
            vmem((COLS, 8, 128), F32),
            dma((12,)),
            dma((3, T)), dma((3, T)), dma((3, T + 1)), dma((3, T + 1)),
            dma, dma, dma, dma,
        ],
        compiler_params=pltpu.CompilerParams(
            collective_id=0, has_side_effects=True, vmem_limit_bytes=VMEM_LIMIT
        ),
    )(*[pltpu.with_memory_space_constraint(x, pltpu.HBM) for x in (
        tiles(w_rec).reshape(2, 8 * J, 128),
        tiles(w_in).reshape(2, 8 * J, 128),
        tiles(gate_pre).reshape(2, T, B, 8, 128),
        cells, layer_in, h_prev, top_grad,
    )])

    def back(w):
        w = (w * scale[0, 0]).astype(BF16)
        return w.reshape(2, J, 2, 4, 128).transpose(0, 1, 3, 2, 4).reshape(2, J, 4, U)

    return back(rec), back(inp), igrad.reshape(T, B, U)


def solution(mesh):
    torus = Mesh(mesh.devices.reshape(4, 2, 4, 4), ("row_0", "row_1", "col_0", "col_1"))
    placed = (
        P(None, ROW, None, COL),
        P(None, ROW, None, COL),
        P(None, None, None, None, COL),
        P(None, None, None, COL),
        P(None, None, None, ROW),
        P(None, None, None, ROW),
        P(None, None, COL),
    )
    return jax.shard_map(
        local,
        mesh=torus,
        in_specs=placed,
        out_specs=(P(None, ROW, None, COL), P(None, ROW, None, COL), P(None, None, COL)),
        check_vma=False,
    )
```

```python
import jax
import jax.numpy as jnp
from jax import lax
from jax.experimental import pallas as pl
from jax.experimental.pallas import tpu as pltpu
from jax.sharding import Mesh
from jax.sharding import PartitionSpec as P

COL = ("col_0", "col_1")
ROW = ("row_0", "row_1")
MESH = pl.DeviceIdType.MESH
F32 = jnp.float32
BF16 = jnp.bfloat16
NORM = 268435456.0
ROWS = 8
COLS = 16
T = 6
B = 64
J = 512
U = 256
VMEM_LIMIT = 50 * 1024 * 1024
OWNERS = 4
PIECE = 16


def dev(r, c):
    return (r // 2, r % 2, c // 4, c % 4)


def push(src, dst, send_sem, recv_sem, where):
    pltpu.make_async_remote_copy(
        src_ref=src, dst_ref=dst, send_sem=send_sem, recv_sem=recv_sem,
        device_id=where, device_id_type=MESH,
    ).start()


def drain(ref, sem):
    pltpu.make_async_copy(ref, ref, sem).wait()


def nn(a, b):
    return jnp.dot(a, b, preferred_element_type=F32)


def tn(a, b):
    return lax.dot_general(a, b, (((0,), (0,)), ((), ())), preferred_element_type=F32)


def kernel(
    w_rec, w_in, gate_pre, cells, layer_in, h_prev, top_grad,
    o_rec, o_in, o_inp,
    wraw, tmp, wk, gp, cl, li, hp, tg, dgs, a_rec, a_in, fac, carry, sq,
    sb, rb, hb, parts,
    ld, rs_s, rs_r, ag_s, ag_r, ps_s, ps_r,
):
    x = lax.axis_index("row_0")
    k = lax.axis_index("row_1")
    r = x * 2 + k
    y = lax.axis_index("col_0")
    z = lax.axis_index("col_1")
    c = y * 4 + z
    me = r * COLS + c
    owner = k == 1
    mine = jnp.logical_and(owner, r == c // 2)
    own = (c % 2) * OWNERS + x
    grads = (a_rec, a_in)

    barrier = pltpu.get_barrier_semaphore()
    for i in range(OWNERS):
        @pl.when(2 * i + 1 != r)
        def _():
            pl.semaphore_signal(barrier, inc=1, device_id=dev(2 * i + 1, c), device_id_type=MESH)

    for i in range(COLS):
        @pl.when(jnp.logical_and(owner, jnp.logical_or(r != c // 2, c != i)))
        def _():
            pl.semaphore_signal(barrier, inc=1, device_id=dev(c // 2, i), device_id_type=MESH)

    last = pl.ds(T - 1, 1)
    rest = pl.ds(0, T - 1)
    loads = [
        (gate_pre.at[1, last], gp.at[1, last]), (cells.at[1], cl.at[1]), (w_rec.at[1], wraw.at[2]),
        (top_grad, tg), (w_in.at[1], wraw.at[3]),
        (w_rec.at[0], wraw.at[0]), (w_in.at[0], wraw.at[1]),
        (gate_pre.at[0], gp.at[0]), (gate_pre.at[1, rest], gp.at[1, rest]), (cells.at[0], cl.at[0]),
        (h_prev, hp), (layer_in, li),
    ]
    copies = [pltpu.make_async_copy(p, q, ld.at[i]) for i, (p, q) in enumerate(loads)]
    for copy in copies:
        copy.start()

    def relayout(m):
        tmp[...] = wraw[m].astype(F32)
        for i in range(8):
            wk[m, pl.ds(i * 128, 128), :] = tmp[pl.ds(i, J, stride=8), :].T.astype(BF16)

    def factors(layer, t):
        for ut in range(2):
            lanes = pl.ds(ut * 128, 128)
            gi = jax.nn.sigmoid(gp[layer, t, :, ut * 4 + 0, :])
            gf = jax.nn.sigmoid(gp[layer, t, :, ut * 4 + 1, :])
            gc = jnp.tanh(gp[layer, t, :, ut * 4 + 2, :])
            go = jax.nn.sigmoid(gp[layer, t, :, ut * 4 + 3, :])
            th = jnp.tanh(cl[layer, t + 1, :, lanes])
            fac[layer, 0, :, lanes] = go * (1.0 - th * th)
            fac[layer, 1, :, lanes] = gc * gi * (1.0 - gi)
            fac[layer, 2, :, lanes] = cl[layer, t, :, lanes] * gf * (1.0 - gf)
            fac[layer, 3, :, lanes] = gi * (1.0 - gc * gc)
            fac[layer, 4, :, lanes] = th * go * (1.0 - go)
            fac[layer, 5, :, lanes] = gf

    def cell(layer, t, hid):
        grad = carry[layer] + hid * fac[layer, 0]
        carry[layer] = grad * fac[layer, 5]
        parts = [grad * fac[layer, 1], grad * fac[layer, 2], grad * fac[layer, 3], hid * fac[layer, 4]]
        for ut in range(2):
            for k in range(4):
                dgs[layer, t, :, pl.ds((ut * 4 + k) * 128, 128)] = (
                    parts[k][:, ut * 128 : ut * 128 + 128].astype(BF16)
                )

    def scatter(ch, s):
        @pl.when(mine)
        def _():
            rb[ch, s, c] = sb[ch, s, own]

        for i in range(2 * OWNERS):
            q = (x + [2, 1, 3, 0][i // 2]) % OWNERS
            h = i % 2
            @pl.when(jnp.logical_or(2 * q + 1 != r, 2 * r + h != c))
            def _():
                push(sb.at[ch, s, h * OWNERS + q], rb.at[ch, s, c], rs_s.at[ch, s], rs_r.at[ch, s],
                     dev(2 * q + 1, 2 * r + h))

    def scatter_sent(ch, s):
        @pl.when(mine)
        def _():
            drain(sb.at[ch, s, pl.ds(0, 2 * OWNERS - 1)], rs_s.at[ch, s])

        @pl.when(jnp.logical_not(mine))
        def _():
            drain(sb.at[ch, s], rs_s.at[ch, s])

    def gather_wait(ch, s):
        @pl.when(owner)
        def _():
            drain(hb.at[ch, s, pl.ds(0, OWNERS - 1)], ag_r.at[ch, s])

        @pl.when(jnp.logical_not(owner))
        def _():
            drain(hb.at[ch, s], ag_r.at[ch, s])

    def gather_sent(ch, s):
        @pl.when(owner)
        def _():
            drain(rb.at[0, 0, pl.ds(0, ROWS - 1)], ag_s.at[ch, s])

    def tree(terms):
        while len(terms) > 1:
            terms = [p + q for p, q in zip(terms[::2], terms[1::2])]
        return terms[0]

    def pass_on(ch, s, to):
        @pl.when(mine)
        def _():
            drain(rb.at[ch, s, pl.ds(0, COLS - 1)], rs_r.at[ch, s])

        @pl.when(jnp.logical_and(owner, jnp.logical_not(mine)))
        def _():
            drain(rb.at[ch, s], rs_r.at[ch, s])

        @pl.when(owner)
        def _():
            hb[ch, to, x] = tree([rb[ch, s, i] for i in range(COLS)])
            for i in [4, 5, 2, 3, 6, 7, 1]:
                at = (x + i // 2) % OWNERS * 2 + (1 + i) % 2
                push(hb.at[ch, to, x], hb.at[ch, to, x], ag_s.at[ch, to], ag_r.at[ch, to], dev(at, c))

    def store(ch, s, prod, add=False):
        for h in range(2):
            at = (ch, s, pl.ds(h * OWNERS, OWNERS))
            piece = prod[:, h * U : h * U + U].reshape(OWNERS, PIECE, U)
            sb[at] = sb[at] + piece if add else piece

    def folded(x):
        return jnp.sum(x.reshape(-1, 64, 128), axis=0)

    def weight_grads(layer, t, square=False):
        two = pl.ds(t, 2)
        for s, left in enumerate((hp, li)):
            for i in range(4):
                prod = tn(left[layer, two].reshape(2 * B, J),
                          dgs[layer, two, :, pl.ds(i * 256, 256)].reshape(2 * B, 256))
                for q in range(2):
                    where = (layer, pl.ds(2 * i + q, J, stride=8))
                    full = grads[s][where] + prod[:, q * 128 : q * 128 + 128]
                    grads[s][where] = full
                    if square:
                        sq[...] = sq[...] + folded(full * full)

    def hidden(ch, d):
        return hb[ch, d].reshape(B, U)

    copies[0].wait()
    copies[1].wait()
    factors(1, T - 1)
    copies[2].wait()
    relayout(2)
    copies[3].wait()
    zero = jnp.zeros((B, U), F32)
    for layer in range(2):
        carry[layer] = zero
        hb[layer, 0] = jnp.zeros((OWNERS, PIECE, U), F32)
    for n in range(6):
        fac[0, n] = zero

    @pl.when(mine)
    def _():
        pl.semaphore_wait(barrier, ROWS - 1 + 2 * OWNERS - 1)

    @pl.when(jnp.logical_and(owner, jnp.logical_not(mine)))
    def _():
        pl.semaphore_wait(barrier, ROWS - 1 + 2 * OWNERS)

    @pl.when(jnp.logical_not(owner))
    def _():
        pl.semaphore_wait(barrier, 2 * OWNERS)

    def diagonal(d, _):
        t1 = T - 1 - d
        t0 = T - d

        @pl.when(d > 0)
        def _():
            gather_wait(0, d)

        cell(1, t1, hidden(0, d) + tg[t1])

        @pl.when(d < T - 1)
        def _():
            store(0, d, nn(dgs[1, t1], wk[2]))
            scatter(0, d)

        @pl.when(d == 0)
        def _():
            copies[4].wait()
            relayout(3)

        store(1, d, nn(dgs[1, t1], wk[3]))

        @pl.when(d > 0)
        def _():
            gather_wait(1, d)

        cell(0, t0, hidden(1, d))

        @pl.when(d > 0)
        def _():
            store(1, d, nn(dgs[0, t0], wk[0]), add=True)

        scatter(1, d)

        @pl.when(d == 0)
        def _():
            for n in range(2):
                for i in range(8):
                    for layer in range(2):
                        grads[n][layer, pl.ds(i * J, J), :] = jnp.zeros((J, 128), F32)
            copies[5].wait()
            relayout(0)
            copies[6].wait()
            relayout(1)
            for copy in copies[7:]:
                copy.wait()

        factors(0, T - 1 - d)

        @pl.when(d < T - 1)
        def _():
            factors(1, T - 2 - d)

        @pl.when(d > 0)
        def _():
            store(2, t0, nn(dgs[0, t0], wk[1]))

        @pl.when(d < T - 1)
        def _():
            pass_on(0, d, d + 1)

        pass_on(1, d, d + 1)

        @pl.when(d > 0)
        def _():
            scatter(2, t0)

        @pl.when(d % 2 == 1)
        def _():
            weight_grads(1, t1)

        @pl.when(jnp.logical_and(d > 0, d % 2 == 0))
        def _():
            weight_grads(0, t0)

        @pl.when(d > 1)
        def _():
            pass_on(2, t0 + 1, t0 + 1)

        return 0

    lax.fori_loop(0, T, diagonal, 0)

    def squares(i, x):
        at = pl.ds(pl.multiple_of(i * 512, 512), 512)
        for n in range(2):
            part = grads[n][1, at, :]
            x = x + folded(part * part)
        return x

    sq[...] = lax.fori_loop(0, 8, squares, jnp.zeros((64, 128), F32))
    gather_wait(1, T)
    cell(0, 0, hidden(1, T))
    store(2, 0, nn(dgs[0, 0], wk[1]))
    scatter(2, 0)
    weight_grads(0, 0, square=True)
    parts[me] = jnp.sum(sq[...], axis=0, keepdims=True)

    for i in (2, 1, 3, 0):
        for n in (2, 1, 3, 0):
            for m in (2, 1, 3, 0):
                for core in range(2):
                    if (i, n, m, core) != (0, 0, 0, 0):
                        there = ((x + i) % 4, (k + core) % 2, (y + n) % 4, (z + m) % 4)
                        push(parts.at[me], parts.at[me], ps_s, ps_r, there)
    pass_on(2, 1, 1)
    pass_on(2, 0, 0)
    drain(parts.at[pl.ds(0, 127)], ps_r)
    sumsq = jnp.sum(jnp.sum(parts[...], axis=0), keepdims=True)
    scale = 1.0 / jnp.maximum(jnp.sqrt(sumsq / NORM), 0.05)

    def finish(i, _):
        at = pl.ds(pl.multiple_of(i * 512, 512), 512)
        for out, full in ((o_rec, a_rec), (o_in, a_in)):
            for layer in range(2):
                out[layer, at, :] = (full[layer, at, :] * scale).astype(BF16)
        return 0

    lax.fori_loop(0, 8, finish, 0)

    def sent(d, _):
        @pl.when(d < T - 1)
        def _():
            scatter_sent(0, d)
            gather_sent(0, d + 1)

        scatter_sent(1, d)
        gather_sent(1, d + 1)
        scatter_sent(2, d)
        gather_sent(2, d)
        return 0

    lax.fori_loop(0, T, sent, 0)
    drain(parts.at[pl.ds(0, 127)], ps_s)
    for t in range(T - 1, -1, -1):
        gather_wait(2, t)
    o_inp[...] = hb[2, pl.ds(0, T)]


def flush(rec, inp, igrad, o_rec, o_in, o_igrad, sem):
    copies = []
    for src, dst in ((rec, o_rec), (inp, o_in)):
        for layer in range(2):
            for i in range(4):
                at = pl.ds(i * 1024, 1024)
                copies.append((src.at[layer, at], dst.at[layer, at]))
    copies.append((igrad, o_igrad))
    copies = [pltpu.make_async_copy(p, q, sem.at[i]) for i, (p, q) in enumerate(copies)]
    for copy in copies:
        copy.start()
    for copy in copies:
        copy.wait()


def local(w_rec, w_in, gate_pre, cells, layer_in, h_prev, top_grad):
    def tiles(w):
        lead = w.shape[:-2]
        axes = tuple(range(len(lead)))
        n = len(lead)
        return w.reshape(lead + (4, 2, 128)).transpose(axes + (n + 1, n, n + 2))

    any_space = pl.BlockSpec(memory_space=pltpu.HBM)
    in_vmem = pl.BlockSpec(memory_space=pltpu.VMEM)
    vmem = pltpu.VMEM
    dma = pltpu.SemaphoreType.DMA
    done = pl.pallas_call(
        kernel,
        out_shape=(
            vmem((2, 8 * J, 128), BF16),
            vmem((2, 8 * J, 128), BF16),
            vmem((T, OWNERS, PIECE, U), F32),
        ),
        in_specs=[any_space] * 7,
        out_specs=(in_vmem,) * 3,
        scratch_shapes=[
            vmem((4, 8 * J, 128), BF16),
            vmem((8 * J, 128), F32),
            vmem((4, 4 * U, J), BF16),
            vmem((2, T, B, 8, 128), F32),
            vmem((2, T + 1, B, U), F32),
            vmem((2, T, B, J), BF16),
            vmem((2, T, B, J), BF16),
            vmem((T, B, U), F32),
            vmem((2, T + 1, B, 4 * U), BF16),
            vmem((2, 8 * J, 128), F32),
            vmem((2, 8 * J, 128), F32),
            vmem((2, 6, B, U), F32),
            vmem((2, B, U), F32),
            vmem((64, 128), F32),
            vmem((3, T, 2 * OWNERS, PIECE, U), F32),
            vmem((3, T, COLS, PIECE, U), F32),
            vmem((3, T + 1, OWNERS, PIECE, U), F32),
            vmem((ROWS * COLS, 1, 128), F32),
            dma((12,)),
            dma((3, T)), dma((3, T)), dma((3, T + 1)), dma((3, T + 1)),
            dma, dma,
        ],
        compiler_params=pltpu.CompilerParams(
            collective_id=0, has_side_effects=True, vmem_limit_bytes=VMEM_LIMIT
        ),
    )(*[pltpu.with_memory_space_constraint(x, pltpu.HBM) for x in (
        tiles(w_rec).reshape(2, 8 * J, 128),
        tiles(w_in).reshape(2, 8 * J, 128),
        tiles(gate_pre).reshape(2, T, B, 8, 128),
        cells, layer_in, h_prev, top_grad,
    )])

    rec, inp, igrad = pl.pallas_call(
        flush,
        out_shape=tuple(jax.ShapeDtypeStruct(x.shape, x.dtype) for x in done),
        in_specs=[in_vmem] * 3,
        out_specs=(any_space,) * 3,
        scratch_shapes=[dma((17,))],
        compiler_params=pltpu.CompilerParams(vmem_limit_bytes=8 * 1024 * 1024),
    )(*[pltpu.with_memory_space_constraint(x, pltpu.VMEM) for x in done])

    def back(w):
        return w.reshape(2, J, 2, 4, 128).transpose(0, 1, 3, 2, 4).reshape(2, J, 4, U)

    return back(rec), back(inp), igrad.reshape(T, B, U)


def solution(mesh):
    torus = Mesh(mesh.devices.reshape(4, 2, 4, 4), ("row_0", "row_1", "col_0", "col_1"))
    placed = (
        P(None, ROW, None, COL),
        P(None, ROW, None, COL),
        P(None, None, None, None, COL),
        P(None, None, None, COL),
        P(None, None, None, ROW),
        P(None, None, None, ROW),
        P(None, None, COL),
    )
    return jax.shard_map(
        local,
        mesh=torus,
        in_specs=placed,
        out_specs=(P(None, ROW, None, COL), P(None, ROW, None, COL), P(None, None, COL)),
        check_vma=False,
    )
```

```python
import itertools

import jax
import jax.numpy as jnp
from jax import lax
from jax.experimental import pallas as pl
from jax.experimental.pallas import tpu as pltpu
from jax.sharding import Mesh
from jax.sharding import PartitionSpec as P

COL = ("col_0", "col_1")
ROW = ("row_0", "row_1")
MESH = pl.DeviceIdType.MESH
F32 = jnp.float32
BF16 = jnp.bfloat16
NORM = 268435456.0
ROWS = 8
COLS = 16
T = 6
B = 64
J = 512
U = 256
VMEM_LIMIT = 50 * 1024 * 1024
OWNERS = 4
PIECE = 16


def dev(r, c):
    return (r // 2, r % 2, c // 4, c % 4)


def push(src, dst, send_sem, recv_sem, where):
    pltpu.make_async_remote_copy(
        src_ref=src, dst_ref=dst, send_sem=send_sem, recv_sem=recv_sem,
        device_id=where, device_id_type=MESH,
    ).start()


def drain(ref, sem):
    pltpu.make_async_copy(ref, ref, sem).wait()


def nn(a, b):
    return jnp.dot(a, b, preferred_element_type=F32)


def tn(a, b):
    return lax.dot_general(a, b, (((0,), (0,)), ((), ())), preferred_element_type=F32)


def kernel(
    w_rec, w_in, gate_pre, cells, layer_in, h_prev, top_grad,
    o_rec, o_in, o_inp,
    wraw, tmp, wk, gp, cl, li, hp, tg, dgs, a_rec, a_in, fac, carry, sq,
    sb, rb, hb, parts,
    ld, rs_s, rs_r, ag_s, ag_r, ps_s, ps_r,
):
    x = lax.axis_index("row_0")
    k = lax.axis_index("row_1")
    r = x * 2 + k
    y = lax.axis_index("col_0")
    z = lax.axis_index("col_1")
    c = y * 4 + z
    me = r * COLS + c
    owner = k == 1
    mine = jnp.logical_and(owner, r == c // 2)
    own = (c % 2) * OWNERS + x
    grads = (a_rec, a_in)

    barrier = pltpu.get_barrier_semaphore()
    for i in range(OWNERS):
        @pl.when(2 * i + 1 != r)
        def _():
            pl.semaphore_signal(barrier, inc=1, device_id=dev(2 * i + 1, c), device_id_type=MESH)

    for i in range(COLS):
        @pl.when(jnp.logical_and(owner, jnp.logical_or(r != c // 2, c != i)))
        def _():
            pl.semaphore_signal(barrier, inc=1, device_id=dev(c // 2, i), device_id_type=MESH)

    last = pl.ds(T - 1, 1)
    rest = pl.ds(0, T - 1)
    ends = pl.ds(T - 1, 2)
    loads = [
        (gate_pre.at[1, last], gp.at[1, last]), (cells.at[1, ends], cl.at[1, ends]), (w_rec.at[1], wraw.at[2]),
        (top_grad, tg), (w_in.at[1], wraw.at[3]),
        (w_rec.at[0], wraw.at[0]), (w_in.at[0], wraw.at[1]),
        (gate_pre.at[0], gp.at[0]), (gate_pre.at[1, rest], gp.at[1, rest]), (cells.at[0], cl.at[0]),
        (cells.at[1, rest], cl.at[1, rest]), (h_prev, hp), (layer_in, li),
    ]
    copies = [pltpu.make_async_copy(p, q, ld.at[i]) for i, (p, q) in enumerate(loads)]
    for copy in copies:
        copy.start()

    def relayout(m):
        tmp[...] = wraw[m].astype(F32)
        for i in range(8):
            wk[m, pl.ds(i * 128, 128), :] = tmp[pl.ds(i, J, stride=8), :].T.astype(BF16)

    def factors(layer, t):
        for ut in range(2):
            lanes = pl.ds(ut * 128, 128)
            gi = jax.nn.sigmoid(gp[layer, t, :, ut * 4 + 0, :])
            gf = jax.nn.sigmoid(gp[layer, t, :, ut * 4 + 1, :])
            gc = jnp.tanh(gp[layer, t, :, ut * 4 + 2, :])
            go = jax.nn.sigmoid(gp[layer, t, :, ut * 4 + 3, :])
            th = jnp.tanh(cl[layer, t + 1, :, lanes])
            fac[layer, 0, :, lanes] = go * (1.0 - th * th)
            fac[layer, 1, :, lanes] = gc * gi * (1.0 - gi)
            fac[layer, 2, :, lanes] = cl[layer, t, :, lanes] * gf * (1.0 - gf)
            fac[layer, 3, :, lanes] = gi * (1.0 - gc * gc)
            fac[layer, 4, :, lanes] = th * go * (1.0 - go)
            fac[layer, 5, :, lanes] = gf

    def cell(layer, t, hid):
        grad = carry[layer] + hid * fac[layer, 0]
        carry[layer] = grad * fac[layer, 5]
        parts = [grad * fac[layer, 1], grad * fac[layer, 2], grad * fac[layer, 3], hid * fac[layer, 4]]
        for ut in range(2):
            for k in range(4):
                dgs[layer, t, :, pl.ds((ut * 4 + k) * 128, 128)] = (
                    parts[k][:, ut * 128 : ut * 128 + 128].astype(BF16)
                )

    def scatter(ch, s, halves=(0, 1)):
        if 1 in halves:
            @pl.when(mine)
            def _():
                rb[ch, s, c] = sb[ch, s, own]

        for i, h in itertools.product((2, 1, 3, 0), halves):
            q = (x + i) % OWNERS
            @pl.when(jnp.logical_or(2 * q + 1 != r, 2 * r + h != c))
            def _():
                push(sb.at[ch, s, h * OWNERS + q], rb.at[ch, s, c], rs_s.at[ch, s], rs_r.at[ch, s],
                     dev(2 * q + 1, 2 * r + h))

    def scatter_sent(ch, s):
        @pl.when(mine)
        def _():
            drain(sb.at[ch, s, pl.ds(0, 2 * OWNERS - 1)], rs_s.at[ch, s])

        @pl.when(jnp.logical_not(mine))
        def _():
            drain(sb.at[ch, s], rs_s.at[ch, s])

    def gather_wait(ch, s):
        @pl.when(owner)
        def _():
            drain(hb.at[ch, s, pl.ds(0, OWNERS - 1)], ag_r.at[ch, s])

        @pl.when(jnp.logical_not(owner))
        def _():
            drain(hb.at[ch, s], ag_r.at[ch, s])

    def gather_sent(ch, s):
        @pl.when(owner)
        def _():
            drain(rb.at[0, 0, pl.ds(0, ROWS - 1)], ag_s.at[ch, s])

    def tree(terms):
        while len(terms) > 1:
            terms = [p + q for p, q in zip(terms[::2], terms[1::2])]
        return terms[0]

    def pass_on(ch, s, to):
        @pl.when(mine)
        def _():
            drain(rb.at[ch, s, pl.ds(0, COLS - 1)], rs_r.at[ch, s])

        @pl.when(jnp.logical_and(owner, jnp.logical_not(mine)))
        def _():
            drain(rb.at[ch, s], rs_r.at[ch, s])

        @pl.when(owner)
        def _():
            hb[ch, to, x] = tree([rb[ch, s, i] for i in range(COLS)])
            for i in [4, 5, 2, 3, 6, 7, 1]:
                at = (x + i // 2) % OWNERS * 2 + (1 + i) % 2
                push(hb.at[ch, to, x], hb.at[ch, to, x], ag_s.at[ch, to], ag_r.at[ch, to], dev(at, c))

    def store(ch, s, left, m, add=False, send=False):
        for h in range(2):
            at = (ch, s, pl.ds(h * OWNERS, OWNERS))
            piece = nn(left, wk[m, :, pl.ds(h * U, U)]).reshape(OWNERS, PIECE, U)
            sb[at] = sb[at] + piece if add else piece
            if send:
                scatter(ch, s, (h,))

    def folded(x):
        return jnp.sum(x.reshape(-1, 64, 128), axis=0)

    def weight_grads(layer, t, square=False):
        two = pl.ds(t, 2)
        for s, left in enumerate((hp, li)):
            for i in range(4):
                prod = tn(left[layer, two].reshape(2 * B, J),
                          dgs[layer, two, :, pl.ds(i * 256, 256)].reshape(2 * B, 256))
                for q in range(2):
                    where = (layer, pl.ds(2 * i + q, J, stride=8))
                    full = grads[s][where] + prod[:, q * 128 : q * 128 + 128]
                    grads[s][where] = full
                    if square:
                        sq[...] = sq[...] + folded(full * full)

    def hidden(ch, d):
        return hb[ch, d].reshape(B, U)

    copies[0].wait()
    copies[1].wait()
    factors(1, T - 1)
    copies[2].wait()
    relayout(2)
    copies[3].wait()
    zero = jnp.zeros((B, U), F32)
    for layer in range(2):
        carry[layer] = zero
        hb[layer, 0] = jnp.zeros((OWNERS, PIECE, U), F32)
    for n in range(6):
        fac[0, n] = zero

    @pl.when(mine)
    def _():
        pl.semaphore_wait(barrier, ROWS - 1 + 2 * OWNERS - 1)

    @pl.when(jnp.logical_and(owner, jnp.logical_not(mine)))
    def _():
        pl.semaphore_wait(barrier, ROWS - 1 + 2 * OWNERS)

    @pl.when(jnp.logical_not(owner))
    def _():
        pl.semaphore_wait(barrier, 2 * OWNERS)

    def diagonal(d, _):
        t1 = T - 1 - d
        t0 = T - d

        @pl.when(d > 0)
        def _():
            gather_wait(0, d)

        cell(1, t1, hidden(0, d) + tg[t1])

        @pl.when(d < T - 1)
        def _():
            store(0, d, dgs[1, t1], 2, send=True)

        @pl.when(d == 0)
        def _():
            copies[4].wait()
            relayout(3)

        store(1, d, dgs[1, t1], 3)

        @pl.when(d > 0)
        def _():
            gather_wait(1, d)

        cell(0, t0, hidden(1, d))

        @pl.when(d > 0)
        def _():
            store(1, d, dgs[0, t0], 0, add=True, send=True)

        @pl.when(d == 0)
        def _():
            scatter(1, d)

        @pl.when(d == 0)
        def _():
            for n in range(2):
                for i in range(8):
                    for layer in range(2):
                        grads[n][layer, pl.ds(i * J, J), :] = jnp.zeros((J, 128), F32)
            copies[5].wait()
            relayout(0)
            copies[6].wait()
            relayout(1)
            for copy in copies[7:]:
                copy.wait()

        factors(0, T - 1 - d)

        @pl.when(d < T - 1)
        def _():
            factors(1, T - 2 - d)

        @pl.when(d > 0)
        def _():
            store(2, t0, dgs[0, t0], 1)

        @pl.when(d % 2 == 1)
        def _():
            weight_grads(1, t1)

        @pl.when(jnp.logical_and(d > 0, d % 2 == 0))
        def _():
            weight_grads(0, t0)

        @pl.when(d < T - 1)
        def _():
            pass_on(0, d, d + 1)

        pass_on(1, d, d + 1)

        @pl.when(d > 0)
        def _():
            scatter(2, t0)

        @pl.when(d > 1)
        def _():
            pass_on(2, t0 + 1, t0 + 1)

        return 0

    lax.fori_loop(0, T, diagonal, 0)

    def squares(i, x):
        at = pl.ds(pl.multiple_of(i * 512, 512), 512)
        for n in range(2):
            part = grads[n][1, at, :]
            x = x + folded(part * part)
        return x

    sq[...] = lax.fori_loop(0, 8, squares, jnp.zeros((64, 128), F32))
    gather_wait(1, T)
    cell(0, 0, hidden(1, T))
    store(2, 0, dgs[0, 0], 1, send=True)
    weight_grads(0, 0, square=True)
    parts[me] = jnp.sum(sq[...], axis=0, keepdims=True)

    for i in (2, 1, 3, 0):
        for n in (2, 1, 3, 0):
            for m in (2, 1, 3, 0):
                for core in range(2):
                    if (i, n, m, core) != (0, 0, 0, 0):
                        there = ((x + i) % 4, (k + core) % 2, (y + n) % 4, (z + m) % 4)
                        push(parts.at[me], parts.at[me], ps_s, ps_r, there)
    pass_on(2, 1, 1)
    pass_on(2, 0, 0)
    drain(parts.at[pl.ds(0, 127)], ps_r)
    sumsq = jnp.sum(jnp.sum(parts[...], axis=0), keepdims=True)
    scale = 1.0 / jnp.maximum(jnp.sqrt(sumsq / NORM), 0.05)

    def finish(i, _):
        at = pl.ds(pl.multiple_of(i * 512, 512), 512)
        for out, full in ((o_rec, a_rec), (o_in, a_in)):
            for layer in range(2):
                out[layer, at, :] = (full[layer, at, :] * scale).astype(BF16)
        return 0

    lax.fori_loop(0, 8, finish, 0)

    def sent(d, _):
        @pl.when(d < T - 1)
        def _():
            scatter_sent(0, d)
            gather_sent(0, d + 1)

        scatter_sent(1, d)
        gather_sent(1, d + 1)
        scatter_sent(2, d)
        gather_sent(2, d)
        return 0

    lax.fori_loop(0, T, sent, 0)
    drain(parts.at[pl.ds(0, 127)], ps_s)
    for t in range(T - 1, -1, -1):
        gather_wait(2, t)
    o_inp[...] = hb[2, pl.ds(0, T)]


def flush(rec, inp, igrad, o_rec, o_in, o_igrad, sem):
    copies = []
    for src, dst in ((rec, o_rec), (inp, o_in)):
        for layer in range(2):
            for i in range(4):
                at = pl.ds(i * 1024, 1024)
                copies.append((src.at[layer, at], dst.at[layer, at]))
    copies.append((igrad, o_igrad))
    copies = [pltpu.make_async_copy(p, q, sem.at[i]) for i, (p, q) in enumerate(copies)]
    for copy in copies:
        copy.start()
    for copy in copies:
        copy.wait()


def local(w_rec, w_in, gate_pre, cells, layer_in, h_prev, top_grad):
    def tiles(w):
        lead = w.shape[:-2]
        axes = tuple(range(len(lead)))
        n = len(lead)
        return w.reshape(lead + (4, 2, 128)).transpose(axes + (n + 1, n, n + 2))

    any_space = pl.BlockSpec(memory_space=pltpu.HBM)
    in_vmem = pl.BlockSpec(memory_space=pltpu.VMEM)
    vmem = pltpu.VMEM
    dma = pltpu.SemaphoreType.DMA
    done = pl.pallas_call(
        kernel,
        out_shape=(
            vmem((2, 8 * J, 128), BF16),
            vmem((2, 8 * J, 128), BF16),
            vmem((T, OWNERS, PIECE, U), F32),
        ),
        in_specs=[any_space] * 7,
        out_specs=(in_vmem,) * 3,
        scratch_shapes=[
            vmem((4, 8 * J, 128), BF16),
            vmem((8 * J, 128), F32),
            vmem((4, 4 * U, J), BF16),
            vmem((2, T, B, 8, 128), F32),
            vmem((2, T + 1, B, U), F32),
            vmem((2, T, B, J), BF16),
            vmem((2, T, B, J), BF16),
            vmem((T, B, U), F32),
            vmem((2, T + 1, B, 4 * U), BF16),
            vmem((2, 8 * J, 128), F32),
            vmem((2, 8 * J, 128), F32),
            vmem((2, 6, B, U), F32),
            vmem((2, B, U), F32),
            vmem((64, 128), F32),
            vmem((3, T, 2 * OWNERS, PIECE, U), F32),
            vmem((3, T, COLS, PIECE, U), F32),
            vmem((3, T + 1, OWNERS, PIECE, U), F32),
            vmem((ROWS * COLS, 1, 128), F32),
            dma((13,)),
            dma((3, T)), dma((3, T)), dma((3, T + 1)), dma((3, T + 1)),
            dma, dma,
        ],
        compiler_params=pltpu.CompilerParams(
            collective_id=0, has_side_effects=True, vmem_limit_bytes=VMEM_LIMIT
        ),
    )(*[pltpu.with_memory_space_constraint(x, pltpu.HBM) for x in (
        tiles(w_rec).reshape(2, 8 * J, 128),
        tiles(w_in).reshape(2, 8 * J, 128),
        tiles(gate_pre).reshape(2, T, B, 8, 128),
        cells, layer_in, h_prev, top_grad,
    )])

    rec, inp, igrad = pl.pallas_call(
        flush,
        out_shape=tuple(jax.ShapeDtypeStruct(x.shape, x.dtype) for x in done),
        in_specs=[in_vmem] * 3,
        out_specs=(any_space,) * 3,
        scratch_shapes=[dma((17,))],
        compiler_params=pltpu.CompilerParams(vmem_limit_bytes=8 * 1024 * 1024),
    )(*[pltpu.with_memory_space_constraint(x, pltpu.VMEM) for x in done])

    def back(w):
        return w.reshape(2, J, 2, 4, 128).transpose(0, 1, 3, 2, 4).reshape(2, J, 4, U)

    return back(rec), back(inp), igrad.reshape(T, B, U)


def solution(mesh):
    torus = Mesh(mesh.devices.reshape(4, 2, 4, 4), ("row_0", "row_1", "col_0", "col_1"))
    placed = (
        P(None, ROW, None, COL),
        P(None, ROW, None, COL),
        P(None, None, None, None, COL),
        P(None, None, None, COL),
        P(None, None, None, ROW),
        P(None, None, None, ROW),
        P(None, None, COL),
    )
    return jax.shard_map(
        local,
        mesh=torus,
        in_specs=placed,
        out_specs=(P(None, ROW, None, COL), P(None, ROW, None, COL), P(None, None, COL)),
        check_vma=False,
    )
```

```python
import itertools

import jax
import jax.numpy as jnp
from jax import lax
from jax.experimental import pallas as pl
from jax.experimental.pallas import tpu as pltpu
from jax.sharding import Mesh
from jax.sharding import PartitionSpec as P

COL = ("col_0", "col_1")
ROW = ("row_0", "row_1")
MESH = pl.DeviceIdType.MESH
F32 = jnp.float32
BF16 = jnp.bfloat16
NORM = 268435456.0
ROWS = 8
COLS = 16
T = 6
B = 64
J = 512
U = 256
VMEM_LIMIT = 50 * 1024 * 1024
OWNERS = 4
PIECE = 16


def dev(r, c):
    return (r // 2, r % 2, c // 4, c % 4)


def push(src, dst, send_sem, recv_sem, where):
    pltpu.make_async_remote_copy(
        src_ref=src, dst_ref=dst, send_sem=send_sem, recv_sem=recv_sem,
        device_id=where, device_id_type=MESH,
    ).start()


def drain(ref, sem):
    pltpu.make_async_copy(ref, ref, sem).wait()


def nn(a, b):
    return jnp.dot(a, b, preferred_element_type=F32)


def tn(a, b):
    return lax.dot_general(a, b, (((0,), (0,)), ((), ())), preferred_element_type=F32)


def kernel(
    w_rec, w_in, gate_pre, cells, layer_in, h_prev, top_grad,
    o_rec, o_in, o_inp,
    wraw, tmp, wk, gp, cl, li, hp, tg, dgs, a_rec, a_in, fac, carry, sq,
    sb, rb, hb, parts,
    ld, rs_s, rs_r, ag_s, ag_r, ps_s, ps_r,
):
    x = lax.axis_index("row_0")
    k = lax.axis_index("row_1")
    r = x * 2 + k
    y = lax.axis_index("col_0")
    z = lax.axis_index("col_1")
    c = y * 4 + z
    me = r * COLS + c
    owner = k == 1
    mine = jnp.logical_and(owner, r == c // 2)
    own = (c % 2) * OWNERS + x
    grads = (a_rec, a_in)

    barrier = pltpu.get_barrier_semaphore()
    for i in range(OWNERS):
        @pl.when(2 * i + 1 != r)
        def _():
            pl.semaphore_signal(barrier, inc=1, device_id=dev(2 * i + 1, c), device_id_type=MESH)

    for i in range(COLS):
        @pl.when(jnp.logical_and(owner, jnp.logical_or(r != c // 2, c != i)))
        def _():
            pl.semaphore_signal(barrier, inc=1, device_id=dev(c // 2, i), device_id_type=MESH)

    last = pl.ds(T - 1, 1)
    rest = pl.ds(0, T - 1)
    ends = pl.ds(T - 1, 2)
    loads = [
        (gate_pre.at[1, last], gp.at[1, last]), (cells.at[1, ends], cl.at[1, ends]), (w_rec.at[1], wraw.at[2]),
        (top_grad, tg), (w_in.at[1], wraw.at[3]),
        (w_rec.at[0], wraw.at[0]), (w_in.at[0], wraw.at[1]),
        (gate_pre.at[0], gp.at[0]), (gate_pre.at[1, rest], gp.at[1, rest]), (cells.at[0], cl.at[0]),
        (cells.at[1, rest], cl.at[1, rest]), (h_prev, hp), (layer_in, li),
    ]
    copies = [pltpu.make_async_copy(p, q, ld.at[i]) for i, (p, q) in enumerate(loads)]
    for copy in copies:
        copy.start()

    def relayout(m):
        tmp[...] = wraw[m].astype(F32)
        for i in range(8):
            wk[m, pl.ds(i * 128, 128), :] = tmp[pl.ds(i, J, stride=8), :].T.astype(BF16)

    def factors(layer, t):
        for ut in range(2):
            lanes = pl.ds(ut * 128, 128)
            gi = jax.nn.sigmoid(gp[layer, t, :, ut * 4 + 0, :])
            gf = jax.nn.sigmoid(gp[layer, t, :, ut * 4 + 1, :])
            gc = jnp.tanh(gp[layer, t, :, ut * 4 + 2, :])
            go = jax.nn.sigmoid(gp[layer, t, :, ut * 4 + 3, :])
            th = jnp.tanh(cl[layer, t + 1, :, lanes])
            fac[layer, 0, :, lanes] = go * (1.0 - th * th)
            fac[layer, 1, :, lanes] = gc * gi * (1.0 - gi)
            fac[layer, 2, :, lanes] = cl[layer, t, :, lanes] * gf * (1.0 - gf)
            fac[layer, 3, :, lanes] = gi * (1.0 - gc * gc)
            fac[layer, 4, :, lanes] = th * go * (1.0 - go)
            fac[layer, 5, :, lanes] = gf

    def cell(layer, t, hid):
        grad = carry[layer] + hid * fac[layer, 0]
        carry[layer] = grad * fac[layer, 5]
        parts = [grad * fac[layer, 1], grad * fac[layer, 2], grad * fac[layer, 3], hid * fac[layer, 4]]
        for ut in range(2):
            for k in range(4):
                dgs[layer, t, :, pl.ds((ut * 4 + k) * 128, 128)] = (
                    parts[k][:, ut * 128 : ut * 128 + 128].astype(BF16)
                )

    def scatter(ch, s, halves=(0, 1)):
        if 1 in halves:
            @pl.when(mine)
            def _():
                rb[ch, s, c] = sb[ch, s, own]

        for i, h in itertools.product((2, 1, 3, 0), halves):
            q = (x + i) % OWNERS
            @pl.when(jnp.logical_or(2 * q + 1 != r, 2 * r + h != c))
            def _():
                push(sb.at[ch, s, h * OWNERS + q], rb.at[ch, s, c], rs_s.at[ch, s], rs_r.at[ch, s],
                     dev(2 * q + 1, 2 * r + h))

    def scatter_sent(ch, s):
        @pl.when(mine)
        def _():
            drain(sb.at[ch, s, pl.ds(0, 2 * OWNERS - 1)], rs_s.at[ch, s])

        @pl.when(jnp.logical_not(mine))
        def _():
            drain(sb.at[ch, s], rs_s.at[ch, s])

    def gather_wait(ch, s):
        @pl.when(owner)
        def _():
            drain(hb.at[ch, s, pl.ds(0, OWNERS - 1)], ag_r.at[ch, s])

        @pl.when(jnp.logical_not(owner))
        def _():
            drain(hb.at[ch, s], ag_r.at[ch, s])

    def gather_sent(ch, s):
        @pl.when(owner)
        def _():
            drain(rb.at[0, 0, pl.ds(0, ROWS - 1)], ag_s.at[ch, s])

    def tree(terms):
        while len(terms) > 1:
            terms = [p + q for p, q in zip(terms[::2], terms[1::2])]
        return terms[0]

    def pass_on(ch, s, to):
        @pl.when(mine)
        def _():
            drain(rb.at[ch, s, pl.ds(0, COLS - 1)], rs_r.at[ch, s])

        @pl.when(jnp.logical_and(owner, jnp.logical_not(mine)))
        def _():
            drain(rb.at[ch, s], rs_r.at[ch, s])

        @pl.when(owner)
        def _():
            hb[ch, to, x] = tree([rb[ch, s, i] for i in range(COLS)])
            for i in [4, 5, 2, 3, 6, 7, 1]:
                at = (x + i // 2) % OWNERS * 2 + (1 + i) % 2
                push(hb.at[ch, to, x], hb.at[ch, to, x], ag_s.at[ch, to], ag_r.at[ch, to], dev(at, c))

    def store(ch, s, left, m, add=False, send=False):
        for h in range(2):
            at = (ch, s, pl.ds(h * OWNERS, OWNERS))
            piece = nn(left, wk[m, :, pl.ds(h * U, U)]).reshape(OWNERS, PIECE, U)
            sb[at] = sb[at] + piece if add else piece
            if send:
                scatter(ch, s, (h,))

    def folded(x):
        return jnp.sum(x.reshape(-1, 64, 128), axis=0)

    def weight_grads(layer, t, square=False):
        two = pl.ds(t, 2)
        for s, left in enumerate((hp, li)):
            for i in range(4):
                prod = tn(left[layer, two].reshape(2 * B, J),
                          dgs[layer, two, :, pl.ds(i * 256, 256)].reshape(2 * B, 256))
                for q in range(2):
                    where = (layer, pl.ds(2 * i + q, J, stride=8))
                    full = grads[s][where] + prod[:, q * 128 : q * 128 + 128]
                    grads[s][where] = full
                    if square:
                        sq[...] = sq[...] + folded(full * full)

    def hidden(ch, d):
        return hb[ch, d].reshape(B, U)

    copies[0].wait()
    copies[1].wait()
    factors(1, T - 1)
    copies[2].wait()
    relayout(2)
    copies[3].wait()
    zero = jnp.zeros((B, U), F32)
    for layer in range(2):
        carry[layer] = zero
        hb[layer, 0] = jnp.zeros((OWNERS, PIECE, U), F32)
    for n in range(6):
        fac[0, n] = zero

    @pl.when(mine)
    def _():
        pl.semaphore_wait(barrier, ROWS - 1 + 2 * OWNERS - 1)

    @pl.when(jnp.logical_and(owner, jnp.logical_not(mine)))
    def _():
        pl.semaphore_wait(barrier, ROWS - 1 + 2 * OWNERS)

    @pl.when(jnp.logical_not(owner))
    def _():
        pl.semaphore_wait(barrier, 2 * OWNERS)

    def diagonal(d, _):
        t1 = T - 1 - d
        t0 = T - d

        @pl.when(d > 0)
        def _():
            gather_wait(0, d)

        cell(1, t1, hidden(0, d) + tg[t1])

        @pl.when(d < T - 1)
        def _():
            store(0, d, dgs[1, t1], 2, send=True)

        @pl.when(d == 0)
        def _():
            copies[4].wait()
            relayout(3)

        store(1, d, dgs[1, t1], 3)

        @pl.when(d > 0)
        def _():
            gather_wait(1, d)

        cell(0, t0, hidden(1, d))

        @pl.when(d > 0)
        def _():
            store(1, d, dgs[0, t0], 0, add=True, send=True)

        @pl.when(d == 0)
        def _():
            scatter(1, d)

        @pl.when(d == 0)
        def _():
            for n in range(2):
                for i in range(8):
                    for layer in range(2):
                        grads[n][layer, pl.ds(i * J, J), :] = jnp.zeros((J, 128), F32)
            copies[5].wait()
            relayout(0)
            copies[6].wait()
            relayout(1)
            for copy in copies[7:]:
                copy.wait()

        factors(0, T - 1 - d)

        @pl.when(d < T - 1)
        def _():
            factors(1, T - 2 - d)

        @pl.when(d > 0)
        def _():
            store(2, t0, dgs[0, t0], 1)

        @pl.when(jnp.logical_and(d > 1, d % 2 == 1))
        def _():
            weight_grads(1, t1)

        @pl.when(jnp.logical_and(d > 0, d % 2 == 0))
        def _():
            weight_grads(0, t0)

        @pl.when(d < T - 1)
        def _():
            pass_on(0, d, d + 1)

        pass_on(1, d, d + 1)

        @pl.when(d > 0)
        def _():
            scatter(2, t0)

        @pl.when(d == 1)
        def _():
            weight_grads(1, t1)

        @pl.when(d == T - 1)
        def _():
            for t in range(T - 1, 1, -1):
                pass_on(2, t, t)

        return 0

    lax.fori_loop(0, T, diagonal, 0)

    def squares(i, x):
        at = pl.ds(pl.multiple_of(i * 512, 512), 512)
        for n in range(2):
            part = grads[n][1, at, :]
            x = x + folded(part * part)
        return x

    sq[...] = lax.fori_loop(0, 8, squares, jnp.zeros((64, 128), F32))
    gather_wait(1, T)
    cell(0, 0, hidden(1, T))
    store(2, 0, dgs[0, 0], 1, send=True)
    weight_grads(0, 0, square=True)
    parts[me] = jnp.sum(sq[...], axis=0, keepdims=True)

    for i in (2, 1, 3, 0):
        for n in (2, 1, 3, 0):
            for m in (2, 1, 3, 0):
                for core in range(2):
                    if (i, n, m, core) != (0, 0, 0, 0):
                        there = ((x + i) % 4, (k + core) % 2, (y + n) % 4, (z + m) % 4)
                        push(parts.at[me], parts.at[me], ps_s, ps_r, there)
    pass_on(2, 1, 1)
    pass_on(2, 0, 0)
    drain(parts.at[pl.ds(0, 127)], ps_r)
    sumsq = jnp.sum(jnp.sum(parts[...], axis=0), keepdims=True)
    scale = 1.0 / jnp.maximum(jnp.sqrt(sumsq / NORM), 0.05)

    def finish(i, _):
        at = pl.ds(pl.multiple_of(i * 512, 512), 512)
        for out, full in ((o_rec, a_rec), (o_in, a_in)):
            for layer in range(2):
                out[layer, at, :] = (full[layer, at, :] * scale).astype(BF16)
        return 0

    lax.fori_loop(0, 8, finish, 0)

    def sent(d, _):
        @pl.when(d < T - 1)
        def _():
            scatter_sent(0, d)
            gather_sent(0, d + 1)

        scatter_sent(1, d)
        gather_sent(1, d + 1)
        scatter_sent(2, d)
        gather_sent(2, d)
        return 0

    lax.fori_loop(0, T, sent, 0)
    drain(parts.at[pl.ds(0, 127)], ps_s)
    for t in range(T - 1, -1, -1):
        gather_wait(2, t)
    o_inp[...] = hb[2, pl.ds(0, T)]


def flush(rec, inp, igrad, o_rec, o_in, o_igrad, sem):
    copies = []
    for src, dst in ((rec, o_rec), (inp, o_in)):
        for layer in range(2):
            for i in range(4):
                at = pl.ds(i * 1024, 1024)
                copies.append((src.at[layer, at], dst.at[layer, at]))
    copies.append((igrad, o_igrad))
    copies = [pltpu.make_async_copy(p, q, sem.at[i]) for i, (p, q) in enumerate(copies)]
    for copy in copies:
        copy.start()
    for copy in copies:
        copy.wait()


def local(w_rec, w_in, gate_pre, cells, layer_in, h_prev, top_grad):
    def tiles(w):
        lead = w.shape[:-2]
        axes = tuple(range(len(lead)))
        n = len(lead)
        return w.reshape(lead + (4, 2, 128)).transpose(axes + (n + 1, n, n + 2))

    any_space = pl.BlockSpec(memory_space=pltpu.HBM)
    in_vmem = pl.BlockSpec(memory_space=pltpu.VMEM)
    vmem = pltpu.VMEM
    dma = pltpu.SemaphoreType.DMA
    done = pl.pallas_call(
        kernel,
        out_shape=(
            vmem((2, 8 * J, 128), BF16),
            vmem((2, 8 * J, 128), BF16),
            vmem((T, OWNERS, PIECE, U), F32),
        ),
        in_specs=[any_space] * 7,
        out_specs=(in_vmem,) * 3,
        scratch_shapes=[
            vmem((4, 8 * J, 128), BF16),
            vmem((8 * J, 128), F32),
            vmem((4, 4 * U, J), BF16),
            vmem((2, T, B, 8, 128), F32),
            vmem((2, T + 1, B, U), F32),
            vmem((2, T, B, J), BF16),
            vmem((2, T, B, J), BF16),
            vmem((T, B, U), F32),
            vmem((2, T + 1, B, 4 * U), BF16),
            vmem((2, 8 * J, 128), F32),
            vmem((2, 8 * J, 128), F32),
            vmem((2, 6, B, U), F32),
            vmem((2, B, U), F32),
            vmem((64, 128), F32),
            vmem((3, T, 2 * OWNERS, PIECE, U), F32),
            vmem((3, T, COLS, PIECE, U), F32),
            vmem((3, T + 1, OWNERS, PIECE, U), F32),
            vmem((ROWS * COLS, 1, 128), F32),
            dma((13,)),
            dma((3, T)), dma((3, T)), dma((3, T + 1)), dma((3, T + 1)),
            dma, dma,
        ],
        compiler_params=pltpu.CompilerParams(
            collective_id=0, has_side_effects=True, vmem_limit_bytes=VMEM_LIMIT
        ),
    )(*[pltpu.with_memory_space_constraint(x, pltpu.HBM) for x in (
        tiles(w_rec).reshape(2, 8 * J, 128),
        tiles(w_in).reshape(2, 8 * J, 128),
        tiles(gate_pre).reshape(2, T, B, 8, 128),
        cells, layer_in, h_prev, top_grad,
    )])

    rec, inp, igrad = pl.pallas_call(
        flush,
        out_shape=tuple(jax.ShapeDtypeStruct(x.shape, x.dtype) for x in done),
        in_specs=[in_vmem] * 3,
        out_specs=(any_space,) * 3,
        scratch_shapes=[dma((17,))],
        compiler_params=pltpu.CompilerParams(vmem_limit_bytes=8 * 1024 * 1024),
    )(*[pltpu.with_memory_space_constraint(x, pltpu.VMEM) for x in done])

    def back(w):
        return w.reshape(2, J, 2, 4, 128).transpose(0, 1, 3, 2, 4).reshape(2, J, 4, U)

    return back(rec), back(inp), igrad.reshape(T, B, U)


def solution(mesh):
    torus = Mesh(mesh.devices.reshape(4, 2, 4, 4), ("row_0", "row_1", "col_0", "col_1"))
    placed = (
        P(None, ROW, None, COL),
        P(None, ROW, None, COL),
        P(None, None, None, None, COL),
        P(None, None, None, COL),
        P(None, None, None, ROW),
        P(None, None, None, ROW),
        P(None, None, COL),
    )
    return jax.shard_map(
        local,
        mesh=torus,
        in_specs=placed,
        out_specs=(P(None, ROW, None, COL), P(None, ROW, None, COL), P(None, None, COL)),
        check_vma=False,
    )
```
